128 devices in a mesh: seq: 16 (over y, x_hi, core), head: 8 (over z, x_lo).
Axes of the slice: x: 4 (x_hi: 2, x_lo: 2; x = x_hi * 2 + x_lo), y: 4, z: 4, core: 2. Of those that a mesh axis runs over, the one named last changes fastest.
Arguments:
- d_bytes: bfloat16 [4096, 8192], P('seq', 'head'), may hold values from -6 to 6
- owner_groups: int32 [16, 16], replicated, may hold values from 0 to 255, as said below
- block_order: int32 [16], replicated, may hold values from 0 to 15, each once
- y_in: bfloat16 [4096, 4096], P('seq'), may hold values from -0.29882812 to 0.29882812
- w_proj: bfloat16 [4096, 8192], P('seq', 'head'), may hold values from -0.0625 to 0.0625
- w_out: bfloat16 [2048, 4096], P('head', 'seq'), may hold values from -0.125 to 0.125
- queries: bfloat16 [4096, 2048], P('seq', 'head'), may hold values from -24 to 24
- keys: bfloat16 [4096, 2048], P('seq', 'head'), may hold values from -24 to 24
- values: bfloat16 [4096, 2048], P('seq', 'head'), may hold values from -6 to 6
- attn_out: bfloat16 [4096, 2048], P('seq', 'head'), may hold values from -0.59765625 to 0.59765625
Outputs:
- layer_grad: bfloat16 [4096, 4096], P('seq', 'head')
- grad_proj: bfloat16 [4096, 8192], P('seq', 'head')
- grad_out: bfloat16 [2048, 4096], P('head', 'seq')
- grad_queries: bfloat16 [4096, 2048], P('seq', 'head')
- grad_keys: bfloat16 [4096, 2048], P('seq', 'head')
- grad_values: bfloat16 [4096, 2048], P('seq', 'head')
The draws below stay inside these ranges and needn't reach their ends.
Inputs may be any that keep to these rules, and one draw needn't show every extreme that they name: `owner_groups`: row o lists the patch groups held by owner o; it holds exactly one group of every seq shard (group g covers patches g * 16 to g * 16 + 15, shard g // 16), and every group appears once. `block_order`: A permutation.
All inputs are finite; a program needn't handle non-finite values.
Results may differ from the reference program's by a relative error of at most 0.03.
Values may be sent and summed in bfloat16 or wider, within the bound.
No kernel may reach another device: no remote copies, remote signals or barrier semaphores. Data moves between devices by JAX's collectives and lax.ppermute only.
A program may use at most 128 MiB of HBM per device.

```python
import math
import jax
import jax.numpy as jnp
from jax import lax

D = 4096
HEADS = 16
HEAD_DIM = 128
PATCH_DEV = 256
BYTE_W = 8192
HW = 2048
PATCHES = 4096
OWNERS = 16
SPLITS = 8
GROUP = 16


def draw_pair(key):
    key_query = jax.random.fold_in(key, 11)
    key_key = jax.random.fold_in(key, 12)
    query_all = jax.random.normal(key_query, (PATCHES, HW), jnp.float32)
    key_all = jax.random.normal(key_key, (PATCHES, HW), jnp.float32)
    query_all = jnp.clip(query_all, -6.0, 6.0)
    key_all = jnp.clip(key_all, -6.0, 6.0)
    return (query_all, key_all)


def draw_queries(key, part):
    return draw_pair(key)[0].astype(jnp.bfloat16)


def draw_keys(key, part):
    return draw_pair(key)[1].astype(jnp.bfloat16)


def draw_owner_groups(key, part):
    shard_keys = jax.random.split(jax.random.fold_in(key, 21), OWNERS)
    placed = jax.vmap(lambda single: jax.random.permutation(single, OWNERS))(shard_keys)
    inverse = jnp.argsort(placed, axis=1).astype(jnp.int32)
    identity = jnp.arange(OWNERS, dtype=jnp.int32)[:, None] * OWNERS + inverse
    table = identity.T
    owner_keys = jax.random.split(jax.random.fold_in(key, 22), OWNERS)
    shuffle = jax.vmap(lambda single: jax.random.permutation(single, OWNERS))(owner_keys).astype(jnp.int32)
    return jnp.take_along_axis(table, shuffle, axis=1).astype(jnp.int32)


def block_scale(own_key, shape, cuts, least, high):
    factor_of = 1.0
    for dim, shards_of in cuts:
        heights = jax.random.uniform(jax.random.fold_in(jax.random.fold_in(own_key, 6), dim), (shards_of,), jnp.float32, least / len(cuts), high / len(cuts))
        factor_of = factor_of * jnp.repeat(jnp.exp(heights), shape[dim] // shards_of).reshape((-1,) + (1,) * (len(shape) - 1 - dim))
    return factor_of


def bell_draw(rng, extent, deviation, limit, shards=(), held_as=jnp.bfloat16):
    result = jax.random.normal(rng, extent, jnp.float32) * deviation
    if len(shards) > 0:
        result = block_scale(rng, extent, shards, -0.22, 0.18) * result
    return jnp.clip(result, min=-limit, max=limit).astype(held_as)


def setup_inputs(seed: int = 0) -> dict:
    arg_keys = jax.random.split(jax.random.key(seed), 11)
    return {
        "d_bytes": bell_draw(arg_keys[0], (PATCHES, BYTE_W), 1.0, 6.0, ((0, 16), (1, 8))),
        "owner_groups": draw_owner_groups(jax.random.fold_in(arg_keys[10], 71), 0),
        "block_order": jax.random.permutation(arg_keys[2], OWNERS).astype(jnp.int32),
        "y_in": bell_draw(arg_keys[3], (PATCHES, D), 0.05, 0.29882812, ((0, 16),)),
        "w_proj": bell_draw(arg_keys[4], (D, BYTE_W), BYTE_W ** -0.5, 0.0625, ((0, 16), (1, 8))),
        "w_out": bell_draw(arg_keys[5], (HW, D), HW ** -0.5, 0.125, ((0, 8), (1, 16))),
        "queries": draw_queries(jax.random.fold_in(arg_keys[10], 71), 0),
        "keys": draw_keys(jax.random.fold_in(arg_keys[10], 71), 0),
        "values": bell_draw(arg_keys[8], (PATCHES, HW), 1.0, 6.0, ((0, 16), (1, 8))),
        "attn_out": bell_draw(arg_keys[9], (PATCHES, HW), 0.1, 0.59765625, ((0, 16), (1, 8))),
    }


def reference(d_bytes, owner_groups, block_order, y_in, w_proj, w_out, queries, keys, values, attn_out):
    flt = jnp.float32
    half = jnp.bfloat16
    flat_ids = owner_groups.reshape(-1)
    inverse = jnp.argsort(flat_ids).astype(jnp.int32)
    owned = d_bytes.reshape(OWNERS * OWNERS, GROUP, BYTE_W)
    natural = jnp.take(owned, inverse, axis=0).reshape(PATCHES, BYTE_W)
    grad_proj = lax.dot_general(y_in, natural, (((0,), (0,)), ((), ())), preferred_element_type=flt).astype(half)
    width = BYTE_W // SPLITS
    summed = jnp.zeros((PATCHES, D), flt)
    for column_group in range(SPLITS):
        lower = column_group * width
        portion = lax.dot_general(natural[:, lower:lower + width], w_proj[:, lower:lower + width], (((1,), (1,)), ((), ())), preferred_element_type=flt)
        summed = summed + lax.optimization_barrier(portion.astype(half)).astype(flt)
    layer_grad = summed.astype(half)
    attn_grad = lax.dot_general(layer_grad, w_out, (((1,), (1,)), ((), ())), preferred_element_type=flt).astype(half)
    out_sum = jnp.zeros((HW, D), flt)
    for shard_index in range(OWNERS):
        lower = shard_index * PATCH_DEV
        portion = lax.dot_general(attn_out[lower:lower + PATCH_DEV], layer_grad[lower:lower + PATCH_DEV], (((0,), (0,)), ((), ())), preferred_element_type=flt)
        out_sum = out_sum + lax.optimization_barrier(portion.astype(half)).astype(flt)
    grad_out = out_sum.astype(half)
    rows = jnp.arange(PATCHES, dtype=jnp.int32)
    position = block_order[rows // PATCH_DEV] * PATCH_DEV + rows % PATCH_DEV
    scale = 1.0 / math.sqrt(HEAD_DIM)
    key_heads = keys.astype(flt).reshape(PATCHES, HEADS, HEAD_DIM)
    value_heads = values.astype(flt).reshape(PATCHES, HEADS, HEAD_DIM)

    def shard(running, shard_index):
        key_sum, value_sum = running
        lower = shard_index * PATCH_DEV
        query_now = lax.dynamic_slice_in_dim(queries, lower, PATCH_DEV, 0).astype(flt).reshape(PATCH_DEV, HEADS, HEAD_DIM)
        grad_now = lax.dynamic_slice_in_dim(attn_grad, lower, PATCH_DEV, 0).astype(flt).reshape(PATCH_DEV, HEADS, HEAD_DIM)
        output_now = lax.dynamic_slice_in_dim(attn_out, lower, PATCH_DEV, 0).astype(flt).reshape(PATCH_DEV, HEADS, HEAD_DIM)
        query_pos = lax.dynamic_slice_in_dim(position, lower, PATCH_DEV, 0)
        allowed = position[None, :] <= query_pos[:, None]
        scores = jnp.einsum('qhd,khd->hqk', query_now, key_heads) * scale
        scores = jnp.where(allowed[None], scores, -jnp.inf)
        highest = lax.optimization_barrier(jnp.max(scores, axis=2, keepdims=True))
        log_total = highest + jnp.log(lax.optimization_barrier(jnp.sum(jnp.exp(scores - highest), axis=2, keepdims=True)))
        weights = jnp.exp(scores - log_total)
        delta = lax.optimization_barrier(jnp.sum(grad_now * output_now, axis=2)).T[:, :, None]
        grad_weights = jnp.einsum('qhd,khd->hqk', grad_now, value_heads)
        grad_scores = lax.optimization_barrier((weights * (grad_weights - delta) * scale).astype(half)).astype(flt)
        weights_low = lax.optimization_barrier(weights.astype(half)).astype(flt)
        grad_query = jnp.einsum('hqk,khd->qhd', grad_scores, key_heads).reshape(PATCH_DEV, HW).astype(half)
        key_term = jnp.einsum('hqk,qhd->khd', grad_scores, query_now).reshape(PATCHES, HW)
        value_term = jnp.einsum('hqk,qhd->khd', weights_low, grad_now).reshape(PATCHES, HW)
        key_sum = key_sum + lax.optimization_barrier(key_term.astype(half)).astype(flt)
        value_sum = value_sum + lax.optimization_barrier(value_term.astype(half)).astype(flt)
        return ((key_sum, value_sum), grad_query)
    start_state = (jnp.zeros((PATCHES, HW), flt), jnp.zeros((PATCHES, HW), flt))
    (key_sum, value_sum), query_grads = lax.scan(shard, start_state, jnp.arange(OWNERS, dtype=jnp.int32))
    grad_queries = query_grads.reshape(PATCHES, HW)
    return (layer_grad, grad_proj, grad_out, grad_queries, key_sum.astype(half), value_sum.astype(half))
```

```python
import math

import jax
import jax.numpy as jnp
from jax import lax
from jax.experimental import pallas as pl
from jax.experimental.pallas import tpu as pltpu
from jax.sharding import Mesh
from jax.sharding import PartitionSpec as P

HEAD_DIM = 128
SIZE = {"y": 4, "xh": 2, "c": 2, "z": 4, "xl": 2}
SCALE = 1.0 / math.sqrt(HEAD_DIM)
flt = jnp.float32
half = jnp.bfloat16


def shift(x, axis, k):
    n = SIZE[axis]
    return lax.ppermute(x, axis, [(i, (i + k) % n) for i in range(n)])


def dyn(x, i, axis=0):
    return lax.dynamic_index_in_dim(x, i, axis, keepdims=False)


def dot(a, b, ca, cb):
    return lax.dot_general(a, b, (((ca,), (cb,)), ((), ())), preferred_element_type=flt)


def dot16(a, b, ca, cb):
    return dot(a, b, ca, cb).astype(half)


def added(*parts):
    total = parts[0].astype(flt)
    for p in parts[1:]:
        total = total + p.astype(flt)
    return total.astype(half)


def one_hot_rows(target, n):
    rows = lax.broadcasted_iota(jnp.int32, (n, target.shape[-1]), 0)
    return (rows == target[..., None, :]).astype(half)


def in_group(first, groups):
    return (first[..., :, None] * 16 + jnp.arange(16, dtype=jnp.int32)).reshape(
        *first.shape[:-1], groups * 16
    )


def nt(a, b):
    return lax.dot_general(a, b, (((1,), (1,)), ((), ())), preferred_element_type=flt)


def nn(a, b):
    return lax.dot_general(a, b, (((1,), (0,)), ((), ())), preferred_element_type=flt)


def tn(a, b):
    return lax.dot_general(a, b, (((0,), (0,)), ((), ())), preferred_element_type=flt)


def allowed_of(bk, bq, n):
    ik = lax.broadcasted_iota(jnp.int32, (n, n), 0)
    iq = lax.broadcasted_iota(jnp.int32, (n, n), 1)
    return (ik + bk * n) <= (iq + bq * n)


def scores(k, q):
    return nt(k, q) * SCALE


def stats_kernel(bq_ref, bk_ref, q_ref, k_ref, out_ref):
    for h in range(2):
        cols = slice(h * HEAD_DIM, (h + 1) * HEAD_DIM)
        for i in range(4):
            m, t = h * 4 + i, 8 + h * 4 + i
            out_ref[m : m + 1, :] = jnp.full((1, 256), -1e30, flt)
            out_ref[t : t + 1, :] = jnp.zeros((1, 256), flt)
            for j in range(4):

                @pl.when(bk_ref[j] <= bq_ref[i])
                def _():
                    s = scores(k_ref[j, :, cols], q_ref[i, :, cols])
                    s = jnp.where(allowed_of(bk_ref[j], bq_ref[i], 256), s, -1e30)
                    before = out_ref[m : m + 1, :]
                    high = jnp.maximum(before, jnp.max(s, axis=0, keepdims=True))
                    total = jnp.sum(jnp.exp(s - high), axis=0, keepdims=True)
                    out_ref[t : t + 1, :] = out_ref[t : t + 1, :] * jnp.exp(before - high) + total
                    out_ref[m : m + 1, :] = high


def backward_kernel(
    bq_ref, bk_ref, c_ref, q_ref, o_ref, mine_ref, other_ref, k_ref, v_ref, stats_ref,
    keep_ref, send_ref, dkv_ref, g_ref, lse_ref, dl_ref, aq, ak, av,
):
    c = c_ref[0]
    for x in range(2):
        g_ref[x * 2 + c] = mine_ref[x]
        g_ref[x * 2 + 1 - c] = other_ref[x]
    high = jnp.max(stats_ref[:, 0:8, :], axis=0)
    total = jnp.sum(stats_ref[:, 8:16, :] * jnp.exp(stats_ref[:, 0:8, :] - high), axis=0)
    lse_ref[...] = high + jnp.log(total)
    ones = jnp.ones((8, HEAD_DIM), flt)
    aq[...] = jnp.zeros_like(aq)
    ak[...] = jnp.zeros_like(ak)
    av[...] = jnp.zeros_like(av)
    for h in range(2):
        cols = slice(h * HEAD_DIM, (h + 1) * HEAD_DIM)
        for i in range(4):
            row = h * 4 + i
            prod = g_ref[i, :, cols].astype(flt) * o_ref[i, :, cols].astype(flt)
            dl_ref[row : row + 1, :] = lax.dot_general(
                ones, prod, (((1,), (1,)), ((), ())),
                precision=lax.Precision.HIGHEST, preferred_element_type=flt,
            )[0:1]
            for j in range(4):

                @pl.when(bk_ref[j] <= bq_ref[i])
                def _():
                    q = q_ref[i, :, cols]
                    g = g_ref[i, :, cols]
                    k = k_ref[j, :, cols]
                    v = v_ref[j, :, cols]
                    w = jnp.exp(scores(k, q) - lse_ref[row : row + 1, :])
                    w = jnp.where(allowed_of(bk_ref[j], bq_ref[i], 256), w, 0.0)
                    d = nt(v, g)
                    ds = (w * (d - dl_ref[row : row + 1, :]) * SCALE).astype(half)
                    av[j, :, cols] += nn(w.astype(half), g)
                    ak[j, :, cols] += nn(ds, q)
                    aq[i, :, cols] += tn(ds, k)

    for x in range(2):
        keep_ref[x] = aq[x * 2 + c].astype(half)
        send_ref[x] = aq[x * 2 + 1 - c].astype(half)
    dkv_ref[:, :, :256] = ak[...].astype(half)
    dkv_ref[:, :, 256:] = av[...].astype(half)


def natural_kernel(c_ref, at_ref, lo_ref, hi_ref, w_ref, nat_ref, keep_ref, send_ref, ws, part):
    for j in range(4):
        for b in range(2):
            ws[:, b * 512 + j * 128 : b * 512 + (j + 1) * 128] = w_ref[j, :, b * 128 : (b + 1) * 128]
    rows = lax.broadcasted_iota(jnp.int32, (512, 512), 0)
    for x in range(2):
        hot = jnp.where(rows == at_ref[x : x + 1, :], 1.0, 0.0).astype(half)
        for b, ref in ((0, lo_ref), (1, hi_ref)):
            full = jnp.concatenate([ref[z * 2 + x] for z in range(4)], axis=0)
            nat_ref[x * 512 : (x + 1) * 512, b * 512 : (b + 1) * 512] = nn(hot, full).astype(half)
        part[x] = nt(nat_ref[x * 512 : (x + 1) * 512, :], ws[...]).astype(half).reshape(2, 256, 256)
    c = c_ref[0]
    for x in range(2):
        keep_ref[x] = part[x, c]
        send_ref[x] = part[x, 1 - c]


def late_kernel(z_ref, nat_ref, o_ref, term_ref, piece_ref):
    at = pl.multiple_of(z_ref[0] * 128, 128)
    for i in range(4):
        for b in range(2):
            piece_ref[i, :, b * 128 : (b + 1) * 128] = nat_ref[
                i * 256 : (i + 1) * 256, pl.ds(at + b * 512, 128)
            ]
    o = o_ref[...].reshape(1024, 256)
    for b in range(2):
        t = tn(o, nat_ref[:, b * 512 : (b + 1) * 512]).astype(half)
        for j in range(4):
            term_ref[j, :, b * 128 : (b + 1) * 128] = t[:, j * 128 : (j + 1) * 128]


def sorted_kernel(z_ref, target_ref, y_ref, out_ref):
    rows = lax.broadcasted_iota(jnp.int32, (256, 256), 0)
    hot = jnp.where(rows == target_ref[...], 1.0, 0.0).astype(half)
    for n in range(4):
        cols = nn(hot, y_ref[:, n * 256 : (n + 1) * 256]).astype(half)
        for j in range(4):
            out_ref[j * 4 + n] = cols[j * 64 : (j + 1) * 64]


VMEM = pl.BlockSpec(memory_space=pltpu.VMEM)
SMEM = pl.BlockSpec(memory_space=pltpu.SMEM)


def third(n):
    return pl.BlockSpec((4, 256, 256), lambda i: (0, 0, n))


def cost(flops):
    return pl.CostEstimate(flops=flops, bytes_accessed=2**21, transcendentals=0)


def shaped(*shape, dtype=half):
    return jax.ShapeDtypeStruct(shape, dtype)


def stats_of(bq, bk, side, kvw):
    return pl.pallas_call(
        stats_kernel,
        grid=(1,),
        out_shape=shaped(16, 256, dtype=flt),
        in_specs=[SMEM, SMEM, third(0), third(0)],
        out_specs=VMEM,
        cost_estimate=cost(3 * 2**30),
    )(bq, bk, side, kvw)


def backward_of(bq, bk, c, side, mine, other, kvw, stats):
    block = (4, 256, 256)
    return pl.pallas_call(
        backward_kernel,
        grid=(1,),
        out_shape=[shaped(2, 256, 256), shaped(2, 256, 256), shaped(4, 256, 512)],
        in_specs=[SMEM] * 3 + [third(0), third(1), VMEM, VMEM, third(0), third(1), VMEM],
        out_specs=[VMEM] * 3,
        scratch_shapes=[pltpu.VMEM(block, half)]
        + [pltpu.VMEM((8, 256), flt)] * 2
        + [pltpu.VMEM(block, flt)] * 3,
        cost_estimate=cost(6 * 2**30),
    )(bq, bk, c, side, side, mine, other, kvw, kvw, stats)


def natural_of(c, at, lo, hi, kvw):
    return pl.pallas_call(
        natural_kernel,
        grid=(1,),
        out_shape=[shaped(1024, 1024), shaped(2, 256, 256), shaped(2, 256, 256)],
        in_specs=[SMEM, VMEM, VMEM, VMEM, third(2)],
        out_specs=[VMEM] * 3,
        scratch_shapes=[pltpu.VMEM((256, 1024), half), pltpu.VMEM((2, 2, 256, 256), half)],
        cost_estimate=cost(2 * 2**30),
    )(c, at, lo, hi, kvw)


def late_of(z, natural, side):
    return pl.pallas_call(
        late_kernel,
        grid=(1,),
        out_shape=[shaped(4, 256, 256)] * 2,
        in_specs=[SMEM, VMEM, third(1)],
        out_specs=[VMEM] * 2,
        cost_estimate=cost(2**30),
    )(z, natural, side)


def sorted_of(z, target, y_in):
    return pl.pallas_call(
        sorted_kernel,
        grid_spec=pltpu.PrefetchScalarGridSpec(
            num_scalar_prefetch=1,
            grid=(1,),
            in_specs=[
                pl.BlockSpec((1, 256), lambda i, z: (0, 0)),
                pl.BlockSpec((256, 1024), lambda i, z: (0, z[0])),
            ],
            out_specs=pl.BlockSpec((16, 64, 256), lambda i, z: (0, 0, 0)),
        ),
        out_shape=shaped(16, 64, 256),
        cost_estimate=cost(2**28),
    )(z, target, y_in)


def exchanged(x, axes):
    return lax.all_to_all(x, axes, 0, 0, tiled=True)


def spread(x, axes, n):
    return exchanged(jnp.broadcast_to(x[None], (n, *x.shape)), axes)


def summed(x):
    return x.astype(flt).sum(axis=0).astype(half)


def target_of(first):
    at = jnp.sum(
        jnp.where(first[:, None] == jnp.arange(16), jnp.arange(16)[:, None], 0), axis=0
    )
    return in_group(at.astype(jnp.int32), 16)[None]


def body(d_bytes, owner_groups, block_order, y_in, w_proj, w_out, queries, keys, values, attn_out):
    y, xh, c, z, xl = (lax.axis_index(a) for a in ("y", "xh", "c", "z", "xl"))
    q = xh * 2 + c
    s = y * 4 + q
    i4 = jnp.arange(4, dtype=jnp.int32)
    i16 = jnp.arange(16, dtype=jnp.int32)
    seq, near, head = ("y", "xh", "c"), ("xh", "c"), ("z", "xl")
    one = lambda t: t.reshape(1).astype(jnp.int32)

    mine = dyn(owner_groups, s) // 16
    place = ((mine // 2) % 2) * 8 + (mine // 4) * 2 + mine % 2
    own = dot16(one_hot_rows(in_group(place, 16), 256), d_bytes, 1, 0)
    r10 = shift(own, "xh", 1)
    w_lo = spread(w_proj[:128], "y", 4).reshape(512, 1024)
    r01 = shift(own, "c", 1)
    r11 = shift(r10, "c", 1)
    rows = jnp.concatenate([own, r01, r10, r11], axis=0)
    w_hi = spread(w_proj[128:], "y", 4).reshape(512, 1024)

    landing = jnp.sum(
        jnp.where(owner_groups[:, :, None] // 16 == i16, owner_groups[:, :, None] % 16, 0), axis=1
    )

    y_own = sorted_of(one(z), target_of(dyn(landing, s, 1)), y_in)
    y_own = exchanged(y_own, seq).reshape(64, 16, 256)
    a = jnp.arange(64, dtype=jnp.int32)
    shard = ((a // 2) % 4) * 4 + ((a // 8) % 2) * 2 + a % 2
    y_own = jnp.take(y_own, shard * 4 + (q ^ (a // 16)), axis=0).reshape(1024, 256)
    y_all = spread(y_own, "z", 4).reshape(4, 1024, 256)

    def reduced(w):
        part = dot16(rows, w, 1, 1).reshape(8, 128, 512)
        block = summed(exchanged(part, head))
        block = exchanged(block.reshape(4, 32, 512), "y").reshape(128, 512)
        return spread(block, head, 8).reshape(8, 128, 512)

    lo, hi = reduced(w_lo), reduced(w_hi)

    src = jnp.arange(32, dtype=jnp.int32)
    owner = ((src // 2) % 4) * 4 + (q ^ (src // 8))
    to_shard = y * 4 + jnp.arange(2, dtype=jnp.int32)[:, None] * 2 + (src % 2)[None, :]
    at = landing.reshape(-1)[owner[None, :] * 16 + to_shard] + (src % 2)[None, :] * 16

    side = spread(jnp.concatenate([queries, attn_out], axis=1), near, 4).reshape(4, 256, 512)
    kvw = spread(jnp.concatenate([keys, values, w_out], axis=1), "y", 4).reshape(4, 256, 768)

    bq = lax.dynamic_slice_in_dim(block_order, y * 4, 4)
    bk = dyn(block_order.reshape(4, 4), q, 1)
    stats = spread(stats_of(bq, bk, side, kvw), near, 4).reshape(4, 16, 256)

    natural, keep, send = natural_of(one(c), in_group(at, 32), lo, hi, kvw)
    grad = added(keep, shift(send, "c", 1))
    grad = added(grad, shift(grad, "xh", 1))
    keep, send, dkv = backward_of(
        bq, bk, one(c), side, grad, shift(grad, "c", 1), kvw, stats
    )
    dkv = summed(exchanged(dkv, "y"))
    dq = added(keep, shift(send, "c", 1))
    dq = added(dyn(dq, xh), shift(dyn(dq, 1 - xh), "xh", 1))

    term, piece = late_of(one(z), natural, side)
    piece = lax.dynamic_slice_in_dim(exchanged(piece, near), xl * 2, 2)
    layer_grad = piece.transpose(1, 0, 2).reshape(256, 512)
    grad_out = summed(exchanged(term, "y"))

    terms = lax.dot_general(
        y_all, rows, (((1,), (0,)), ((), ())), preferred_element_type=flt
    ).astype(half)
    grad_proj = summed(exchanged(terms, "y"))
    return layer_grad, grad_proj, grad_out, dq, dkv[:, :256], dkv[:, 256:]


def solution(mesh):
    axes = ("y", "xh", "c", "z", "xl")
    finer = Mesh(mesh.devices.reshape([SIZE[a] for a in axes]), axes)
    seq, head = ("y", "xh", "c"), ("z", "xl")
    both = P(seq, head)
    placed = (both, P(), P(), P(seq, None), both, P(head, seq), both, both, both, both)
    return jax.shard_map(
        body,
        mesh=finer,
        in_specs=placed,
        out_specs=(both, both, P(head, seq), both, both, both),
        check_vma=False,
    )
```

```python
import math

import jax
import jax.numpy as jnp
from jax import lax
from jax.experimental import pallas as pl
from jax.experimental.pallas import tpu as pltpu
from jax.sharding import Mesh
from jax.sharding import PartitionSpec as P


HEAD_DIM = 128
SIZE = {"y": 4, "xh": 2, "c": 2, "z": 4, "xl": 2}
SCALE = 1.0 / math.sqrt(HEAD_DIM)
LOG2_E = math.log2(math.e)
flt = jnp.float32
half = jnp.bfloat16


def shift(x, axis, k):
    n = SIZE[axis]
    return lax.ppermute(x, axis, [(i, (i + k) % n) for i in range(n)])


def dyn(x, i, axis=0):
    return lax.dynamic_index_in_dim(x, i, axis, keepdims=False)


def dot(a, b, ca, cb):
    return lax.dot_general(a, b, (((ca,), (cb,)), ((), ())), preferred_element_type=flt)


def dot16(a, b, ca, cb):
    return dot(a, b, ca, cb).astype(half)


def added(*parts):
    total = parts[0].astype(flt)
    for p in parts[1:]:
        total = total + p.astype(flt)
    return total.astype(half)


def one_hot_rows(target, n):
    rows = lax.broadcasted_iota(jnp.int32, (n, target.shape[-1]), 0)
    return (rows == target[..., None, :]).astype(half)


def in_group(first, groups):
    return (first[..., :, None] * 16 + jnp.arange(16, dtype=jnp.int32)).reshape(
        *first.shape[:-1], groups * 16
    )


def nt(a, b):
    return lax.dot_general(a, b, (((1,), (1,)), ((), ())), preferred_element_type=flt)


def nn(a, b):
    return lax.dot_general(a, b, (((1,), (0,)), ((), ())), preferred_element_type=flt)


def tn(a, b):
    return lax.dot_general(a, b, (((0,), (0,)), ((), ())), preferred_element_type=flt)


def allowed_of(bk, bq, n):
    ik = lax.broadcasted_iota(jnp.int32, (n, n), 0)
    iq = lax.broadcasted_iota(jnp.int32, (n, n), 1)
    return (ik + bk * n) <= (iq + bq * n)


def stats_kernel(bq_ref, bk_ref, q0, q1, q2, q3, k0, k1, k2, k3, out_ref, e_ref, s_ref, e_now, sems):
    def leave(n):
        return pltpu.make_async_copy(e_now.at[n], e_ref.at[pl.ds(n * 4, 4)], sems.at[n])

    for h in range(2):
        cols = slice(h * HEAD_DIM, (h + 1) * HEAD_DIM)
        for i, q_ref in enumerate((q0, q1, q2, q3)):
            m, t = h * 4 + i, 8 + h * 4 + i
            out_ref[m : m + 1, :] = jnp.full((1, 256), -1e30, flt)
            out_ref[t : t + 1, :] = jnp.zeros((1, 256), flt)
            for j, k_ref in enumerate((k0, k1, k2, k3)):

                @pl.when(bk_ref[j] <= bq_ref[i])
                def _():
                    s = nt(k_ref[:, cols], q_ref[:, cols])
                    s = jnp.where(allowed_of(bk_ref[j], bq_ref[i], 256), s, -1e30)
                    s_ref[j] = s
                    out_ref[m : m + 1, :] = jnp.maximum(
                        out_ref[m : m + 1, :], jnp.max(s, axis=0, keepdims=True)
                    )

            for j in range(4):

                @pl.when(bk_ref[j] <= bq_ref[i])
                def _():
                    e = jnp.exp2((s_ref[j] - out_ref[m : m + 1, :]) * (SCALE * LOG2_E))
                    out_ref[t : t + 1, :] += jnp.sum(e, axis=0, keepdims=True)
                    e_now[m, j] = e.astype(half)

            leave(m).start()

    for n in range(8):
        leave(n).wait()


def backward_kernel(
    bq_ref, bk_ref, q0, q1, q2, q3, o0, o1, o2, o3, g_mine, g_other, k0, k1, k2, k3,
    v0, v1, v2, v3, s0, s1, s2, s3, e_ref, q_keep, q_near, d0, d1, d2, d3, f_ref, dl_ref, kt, aq, ak, av, e_now, sems,
):
    def fetch(n):
        return pltpu.make_async_copy(e_ref.at[pl.ds(n * 4, 4)], e_now.at[n], sems.at[n])

    for n in range(8):
        fetch(n).start()
    for h in range(2):
        for i in range(4):
            held = [(r, h * 4 + (i ^ n)) for n, r in enumerate((s0, s1, s2, s3))]
            highs = [r[a : a + 1, :] for r, a in held]
            high = jnp.maximum(jnp.maximum(highs[0], highs[1]), jnp.maximum(highs[2], highs[3]))
            ratio = [jnp.exp2((m - high) * (SCALE * LOG2_E)) for m in highs]
            total = sum(r[8 + a : 9 + a, :] * n for (r, a), n in zip(held, ratio))
            f_ref[h * 4 + i : h * 4 + i + 1, :] = ratio[0] / total
    ones = jnp.ones((8, HEAD_DIM), flt)
    aq[...] = jnp.zeros_like(aq)
    ak[...] = jnp.zeros_like(ak)
    av[...] = jnp.zeros_like(av)
    for h in range(2):
        cols = slice(h * HEAD_DIM, (h + 1) * HEAD_DIM)
        for j, k_ref in enumerate((k0, k1, k2, k3)):
            kt[j] = k_ref[:, cols].T
        for i, (q_ref, o_ref) in enumerate(((q0, o0), (q1, o1), (q2, o2), (q3, o3))):
            row = h * 4 + i
            g_ref = (g_mine, g_other)[i % 2]
            prod = g_ref[i // 2, :, cols].astype(flt) * o_ref[:, cols].astype(flt)
            dl_ref[row : row + 1, :] = lax.dot_general(
                ones, prod, (((1,), (1,)), ((), ())),
                precision=lax.Precision.HIGHEST, preferred_element_type=flt,
            )[0:1]
            fetch(row).wait()
            for j, v_ref in enumerate((v0, v1, v2, v3)):

                @pl.when(bk_ref[j] <= bq_ref[i])
                def _():
                    g = g_ref[i // 2, :, cols]
                    w = e_now[row, j].astype(flt) * f_ref[row : row + 1, :]
                    d = nt(v_ref[:, cols], g)
                    ds = (w * (d - dl_ref[row : row + 1, :])).astype(half)
                    av[j, :, cols] += nn(w.astype(half), g)
                    ak[j, :, cols] += nn(ds, q_ref[:, cols])
                    aq[row] += nn(kt[j], ds)

    for h in range(2):
        cols = slice(h * HEAD_DIM, (h + 1) * HEAD_DIM)
        for i in range(4):
            got = aq[h * 4 + i].T * SCALE
            if i % 2:
                q_near[i // 2, :, cols] = got.astype(half)
            else:
                q_keep[i // 2, :, cols] = got
    for j, d_ref in enumerate((d0, d1, d2, d3)):
        d_ref[:, :256] = (ak[j] * SCALE).astype(half)
        d_ref[:, 256:] = av[j].astype(half)


def parts_kernel(r0, r1, r2, r3, wa, wb, out_ref):
    for b, w in enumerate((wa, wb)):
        for i, r in enumerate((r0, r1, r2, r3)):
            part = nt(r[...], w[...]).astype(half)
            out_ref[2 * i, :, b * 256 : (b + 1) * 256] = part[:128]
            out_ref[2 * i + 1, :, b * 256 : (b + 1) * 256] = part[128:]


def sums_kernel(y_ref, parts_ref, o0, o1, o2, o3):
    for n, out in enumerate((o0, o1, o2, o3)):
        at = pl.multiple_of(((y_ref[0] + n) % 4) * 32, 32)
        out[...] = jnp.sum(parts_ref[:, pl.ds(at, 32), :].astype(flt), axis=0).astype(half)


def copies_kernel(p0, p1, p2, p3, out_ref):
    for h in range(8):
        for n, p in enumerate((p0, p1, p2, p3)):
            out_ref[h, n * 32 : (n + 1) * 32, :] = p[...]


def natural_kernel(xh_ref, at_ref, lo_ref, hi_ref, w0, w1, w2, w3, nat_ref, keep_ref, send_ref, ws, full):
    for p, w in enumerate((w0, w1, w2, w3)):
        ws[:, p * 256 : (p + 1) * 256] = w[...]
    rows = lax.broadcasted_iota(jnp.int32, (512, 512), 0)
    for x in range(2):
        for z in range(4):
            at = z * 2 + (xh_ref[0] ^ x)
            for n in range(4):
                for ref, blocks in ((lo_ref, LOW), (hi_ref, HIGH)):
                    for b, m in enumerate(blocks):
                        p = (n + m) % 4
                        full[z * 128 + n * 32 : z * 128 + (n + 1) * 32, p * 256 : (p + 1) * 256] = ref[
                            at, n * 32 : (n + 1) * 32, b * 256 : (b + 1) * 256
                        ]
        hot = jnp.where(rows == at_ref[x : x + 1, :], 1.0, 0.0).astype(half)
        nat = nn(hot, full[...]).astype(half)
        nat_ref[x * 512 : (x + 1) * 512, :] = nat
        part = nt(nat, ws[...]).astype(half)
        keep_ref[x] = part[:256]
        send_ref[x] = part[256:]


def late_kernel(turn_ref, nat_ref, o0, o1, o2, o3, t0, t1, t2, t3, near_ref, other_ref, o):
    at = pl.multiple_of(turn_ref[0] * 256, 256)
    for x in range(2):
        near_ref[x] = nat_ref[x * 512 : x * 512 + 256, pl.ds(at, 256)]
        other_ref[x] = nat_ref[x * 512 + 256 : (x + 1) * 512, pl.ds(at, 256)]
    for i, r in enumerate((o0, o1, o2, o3)):
        o[i * 256 : (i + 1) * 256, :] = r[...]
    for n, t in enumerate((t0, t1, t2, t3)):
        p = (4 - n) % 4
        t[...] = tn(o[...], nat_ref[:, p * 256 : (p + 1) * 256]).astype(half)


def terms_kernel(at_ref, d0, d1, d2, d3, y0, y1, y2, y3, keep0, keep1, send):
    def part(a, b):
        at = pl.multiple_of((at_ref[0] ^ a) * 512 + (at_ref[1] ^ b) * 256, 256)
        total = None
        for d, r in ((d0, y0), (d1, y1), (d2, y2), (d3, y3)):
            now = tn(r[:, pl.ds(at, 256)], d[...])
            total = now if total is None else total + now
        return total.astype(half)

    keep0[...] = part(0, 0)
    keep1[...] = part(1, 0)
    send[0] = part(0, 1)
    send[1] = part(1, 1)


VMEM = pl.BlockSpec(memory_space=pltpu.VMEM)
SMEM = pl.BlockSpec(memory_space=pltpu.SMEM)
ANY = pl.BlockSpec(memory_space=pl.ANY)
HBM = pl.BlockSpec(memory_space=pltpu.HBM)


def columns(n):
    return [pl.BlockSpec((256, 256), lambda i: (0, n))] * 4


def cost(flops):
    return pl.CostEstimate(flops=flops, bytes_accessed=2**21, transcendentals=0)


def shaped(*shape, dtype=half):
    return jax.ShapeDtypeStruct(shape, dtype)


def call(kernel, out_shape, in_specs, flops, scratch=()):
    many = isinstance(out_shape, list)
    return pl.pallas_call(
        kernel,
        grid=(1,),
        out_shape=out_shape,
        in_specs=in_specs,
        out_specs=[VMEM] * len(out_shape) if many else VMEM,
        scratch_shapes=list(scratch),
        cost_estimate=cost(flops),
        compiler_params=pltpu.CompilerParams(vmem_limit_bytes=48 * 2**20),
    )


def stats_of(bq, bk, sides, kvw):
    return pl.pallas_call(
        stats_kernel,
        grid=(1,),
        out_shape=[shaped(16, 256, dtype=flt), shaped(32, 256, 256)],
        in_specs=[SMEM] * 2 + columns(0) + columns(0),
        out_specs=[VMEM, HBM],
        scratch_shapes=[
            pltpu.VMEM((4, 256, 256), flt),
            pltpu.VMEM((8, 4, 256, 256), half),
            pltpu.SemaphoreType.DMA((8,)),
        ],
        cost_estimate=cost(3 * 2**30),
        compiler_params=pltpu.CompilerParams(vmem_limit_bytes=48 * 2**20),
    )(bq, bk, *sides, *kvw)


def backward_of(bq, bk, sides, mine, other, kvw, stats, e):
    return call(
        backward_kernel,
        [shaped(2, 256, 256, dtype=flt), shaped(2, 256, 256)] + [shaped(256, 512)] * 4,
        [SMEM] * 2 + columns(0) + columns(1) + [VMEM] * 2 + columns(0) + columns(1) + [VMEM] * 4 + [ANY],
        6 * 2**30,
        [pltpu.VMEM((8, 256), flt)] * 2
        + [pltpu.VMEM((4, 128, 256), half), pltpu.VMEM((8, 128, 256), flt)]
        + [pltpu.VMEM((4, 256, 256), flt)] * 2
        + [pltpu.VMEM((8, 4, 256, 256), half), pltpu.SemaphoreType.DMA((8,))],
    )(bq, bk, *sides, *sides, mine, other, *kvw, *kvw, *stats, e)


def parts_of(rows, wa, wb):
    return call(parts_kernel, shaped(8, 128, 512), [VMEM] * 6, 2**30)(*rows, wa, wb)


def sums_of(y, parts):
    return call(sums_kernel, [shaped(32, 512)] * 4, [SMEM, VMEM], 2**26)(y, parts)


def copies_of(pieces):
    return call(copies_kernel, shaped(8, 128, 512), [VMEM] * 4, 2**26)(*pieces)


def natural_of(xh, at, lo, hi, kvw):
    return call(
        natural_kernel,
        [shaped(1024, 1024), shaped(2, 256, 256), shaped(2, 256, 256)],
        [SMEM] + [VMEM] * 3 + columns(2),
        2 * 2**30,
        [pltpu.VMEM((256, 1024), half), pltpu.VMEM((512, 1024), half)],
    )(xh, at, lo, hi, *kvw)


def late_of(turn, natural, sides):
    return call(
        late_kernel,
        [shaped(256, 256)] * 4 + [shaped(2, 256, 256)] * 2,
        [SMEM, VMEM] + columns(1),
        2**30,
        [pltpu.VMEM((1024, 256), half)],
    )(turn, natural, *sides)


def terms_of(at, ds, ys):
    return call(
        terms_kernel,
        [shaped(256, 1024)] * 2 + [shaped(2, 256, 1024)],
        [SMEM] + [VMEM] * 8,
        3 * 2**30,
    )(at, *ds, *ys)


LOW, HIGH = (0, 1), (3, 2)


def exchanged(x, axes):
    return lax.all_to_all(x, axes, 0, 0, tiled=True)


def moved(x, axis, k=1):
    return shift(x, axis, k)


def around(xs, axis, sign=1):
    xs = list(xs) if isinstance(xs, (list, tuple)) else [xs] * 4
    got = {m: moved(xs[m], axis, sign * m) for m in (1, 3, 2)}
    return [xs[0], got[1], got[2], got[3]]


def after(first, parts):
    return lax.optimization_barrier((first, *parts))[1:]


def body(d_bytes, owner_groups, block_order, y_in, w_proj, w_out, queries, keys, values, attn_out):
    y, xh, c, z, xl = (lax.axis_index(a) for a in ("y", "xh", "c", "z", "xl"))
    q = xh * 2 + c
    s = y * 4 + q
    i4 = jnp.arange(4, dtype=jnp.int32)
    i16 = jnp.arange(16, dtype=jnp.int32)
    seq, head = ("y", "xh", "c"), ("z", "xl")
    one = lambda t: t.reshape(1).astype(jnp.int32)

    mine = dyn(owner_groups, s) // 16
    place = ((mine // 2) % 2) * 8 + (mine // 4) * 2 + mine % 2
    own = dot16(one_hot_rows(in_group(place, 16), 256), d_bytes, 1, 0)
    r10 = moved(own, "xh")
    w_rel = around(w_proj, "y")
    r01 = moved(own, "c")
    r11 = moved(r10, "c")
    rows = (own, r01, r10, r11)

    landing = jnp.sum(
        jnp.where(owner_groups[:, :, None] // 16 == i16, owner_groups[:, :, None] % 16, 0), axis=1
    )

    by_shard = dot16(one_hot_rows(in_group(mine, 16), 256), d_bytes, 1, 0)
    by_owner = exchanged(by_shard.reshape(16, 16, 1024), seq).reshape(256, 1024)
    kept = dot16(one_hot_rows(in_group(dyn(landing, s, 1), 16), 256), by_owner, 1, 0)
    d_near = around(kept, "y")
    y_cut = [lax.dynamic_slice_in_dim(y_in, ((y + n) % 4) * 1024, 1024, 1) for n in range(4)]

    def reduced(part):
        pieces = sums_of(one(y), exchanged(part, head))
        pieces = around(pieces, "y")
        return exchanged(copies_of(pieces), head)

    part = parts_of(rows, *[w_rel[m] for m in HIGH])
    part, *y_cut = lax.optimization_barrier((part, *y_cut))
    lo, hi = reduced(parts_of(rows, *[w_rel[m] for m in LOW])), reduced(part)
    y_near = around(y_cut, "y")

    src = jnp.arange(32, dtype=jnp.int32)
    owner = ((y - (src // 2) % 4) % 4) * 4 + (q ^ (src // 8))
    to_shard = y * 4 + (xh ^ jnp.arange(2, dtype=jnp.int32))[:, None] * 2 + (src % 2)[None, :]
    at = landing.reshape(-1)[owner[None, :] * 16 + to_shard] + ((src % 2) ^ c)[None, :] * 16

    side = jnp.concatenate([queries, attn_out], axis=1)
    s10 = moved(side, "xh")
    sides = (side, moved(side, "c"), s10, moved(s10, "c"))
    kvw = around(jnp.concatenate([keys, values, w_out], axis=1), "y")

    bq = block_order[y * 4 + (q ^ i4)]
    bk = block_order[((y - i4) % 4) * 4 + q]
    stats, e = stats_of(bq, bk, sides, kvw)
    far = lax.ppermute(stats, ("xh", "c"), [(i, i ^ 3) for i in range(4)])
    stats = (stats, moved(stats, "c"), moved(stats, "xh"), far)

    natural, keep, send = natural_of(one(xh), in_group(at, 32), lo, hi, kvw)
    grad = added(keep, moved(send, "c"))
    grad = added(grad, moved(grad, "xh")[::-1])
    q_keep, q_near, *dkv = backward_of(bq, bk, sides, grad, moved(grad, "c"), kvw, stats, e)
    dkv = around(dkv, "y", -1)
    q_far = moved(q_near, "c")
    q_send = added(q_keep[1], q_far[1])
    q_got = moved(q_send, "xh")
    dq = added(q_keep[0], q_far[0], q_got)

    *term, near, other = late_of(one((y - z) % 4), natural, sides)
    other = moved(other, "c")
    both = [
        jnp.concatenate(
            [jnp.where(c == 0, near[x], other[x]), jnp.where(c == 0, other[x], near[x])], axis=1
        )
        for x in range(2)
    ]
    both[1] = lax.ppermute(both[1], ("xh", "xl"), [(0, 2), (3, 1)])
    layer_grad = jnp.where(xh == xl, *both)
    grad_out = added(*after(layer_grad, around(term, "y")))

    keep0, keep1, send = terms_of(jnp.stack([xh, c]).astype(jnp.int32), d_near, y_near)
    got = moved(send, "c")
    far = moved(added(keep1, got[1]), "xh")
    grad_proj = added(*after(layer_grad, (keep0, got[0], far)))
    dkv = after(grad_proj, dkv)
    grad_keys = added(*[t[:, :256] for t in dkv])
    grad_values = added(*[t[:, 256:] for t in dkv])
    return layer_grad, grad_proj, grad_out, dq, grad_keys, grad_values


def solution(mesh):
    axes = ("y", "xh", "c", "z", "xl")
    finer = Mesh(mesh.devices.reshape([SIZE[a] for a in axes]), axes)
    seq, head = ("y", "xh", "c"), ("z", "xl")
    both = P(seq, head)
    placed = (both, P(), P(), P(seq, None), both, P(head, seq), both, both, both, both)
    return jax.shard_map(
        body,
        mesh=finer,
        in_specs=placed,
        out_specs=(both, both, P(head, seq), both, both, both),
        check_vma=False,
    )
```

```python
import math

import jax
import jax.numpy as jnp
from jax import lax
from jax.experimental import pallas as pl
from jax.experimental.pallas import tpu as pltpu
from jax.sharding import Mesh
from jax.sharding import PartitionSpec as P


HEAD_DIM = 128
SIZE = {"y": 4, "xh": 2, "c": 2, "z": 4, "xl": 2}
SCALE = 1.0 / math.sqrt(HEAD_DIM)
LOG2_E = math.log2(math.e)
flt = jnp.float32
half = jnp.bfloat16


def shift(x, axis, k):
    n = SIZE[axis]
    return lax.ppermute(x, axis, [(i, (i + k) % n) for i in range(n)])


def dyn(x, i, axis=0):
    return lax.dynamic_index_in_dim(x, i, axis, keepdims=False)


def dot(a, b, ca, cb):
    return lax.dot_general(a, b, (((ca,), (cb,)), ((), ())), preferred_element_type=flt)


def dot16(a, b, ca, cb):
    return dot(a, b, ca, cb).astype(half)


def added(*parts):
    total = parts[0].astype(flt)
    for p in parts[1:]:
        total = total + p.astype(flt)
    return total.astype(half)


def one_hot_rows(target, n):
    rows = lax.broadcasted_iota(jnp.int32, (n, target.shape[-1]), 0)
    return (rows == target[..., None, :]).astype(half)


def in_group(first, groups):
    return (first[..., :, None] * 16 + jnp.arange(16, dtype=jnp.int32)).reshape(
        *first.shape[:-1], groups * 16
    )


def nt(a, b):
    return lax.dot_general(a, b, (((1,), (1,)), ((), ())), preferred_element_type=flt)


def nn(a, b):
    return lax.dot_general(a, b, (((1,), (0,)), ((), ())), preferred_element_type=flt)


def tn(a, b):
    return lax.dot_general(a, b, (((0,), (0,)), ((), ())), preferred_element_type=flt)


def allowed_of(bk, bq, n):
    ik = lax.broadcasted_iota(jnp.int32, (n, n), 0)
    iq = lax.broadcasted_iota(jnp.int32, (n, n), 1)
    return (ik + bk * n) <= (iq + bq * n)


def stats_kernel(bq_ref, bk_ref, q0, q1, q2, q3, k0, k1, k2, k3, out_ref, e_ref, s_ref, e_now, sems):
    def leave(n):
        return pltpu.make_async_copy(e_now.at[n], e_ref.at[pl.ds(n * 4, 4)], sems.at[n])

    heads = [slice(h * HEAD_DIM, (h + 1) * HEAD_DIM) for h in range(2)]
    out_ref[0:8, :] = jnp.full((8, 256), -1e30, flt)
    out_ref[8:16, :] = jnp.zeros((8, 256), flt)
    for i, q_ref in enumerate((q0, q1, q2, q3)):
        for j, k_ref in enumerate((k0, k1, k2, k3)):

            @pl.when(bk_ref[j] <= bq_ref[i])
            def _():
                seen = allowed_of(bk_ref[j], bq_ref[i], 256)
                for h, cols in enumerate(heads):
                    m = h * 4 + i
                    s = jnp.where(seen, nt(k_ref[:, cols], q_ref[:, cols]), -1e30)
                    s_ref[h * 4 + j] = s
                    out_ref[m : m + 1, :] = jnp.maximum(
                        out_ref[m : m + 1, :], jnp.max(s, axis=0, keepdims=True)
                    )

        for j in range(4):

            @pl.when(bk_ref[j] <= bq_ref[i])
            def _():
                for h in range(2):
                    m, t = h * 4 + i, 8 + h * 4 + i
                    e = jnp.exp2((s_ref[h * 4 + j] - out_ref[m : m + 1, :]) * (SCALE * LOG2_E))
                    out_ref[t : t + 1, :] += jnp.sum(e, axis=0, keepdims=True)
                    e_now[m, j] = e.astype(half)

        for h in range(2):
            leave(h * 4 + i).start()

    for n in range(8):
        leave(n).wait()


def backward_kernel(
    bq_ref, bk_ref, q0, q1, q2, q3, o0, o1, o2, o3, g_mine, g_other, k0, k1, k2, k3,
    v0, v1, v2, v3, s0, s1, s2, s3, e_ref, q_keep, q_near, d0, d1, d2, d3, f_ref, dl_ref, kt, aq, ak, av, e_now, sems,
):
    def fetch(n):
        return pltpu.make_async_copy(e_ref.at[pl.ds(n * 4, 4)], e_now.at[n], sems.at[n])

    for n in range(8):
        fetch(n).start()
    for h in range(2):
        for i in range(4):
            held = [(r, h * 4 + (i ^ n)) for n, r in enumerate((s0, s1, s2, s3))]
            highs = [r[a : a + 1, :] for r, a in held]
            high = jnp.maximum(jnp.maximum(highs[0], highs[1]), jnp.maximum(highs[2], highs[3]))
            ratio = [jnp.exp2((m - high) * (SCALE * LOG2_E)) for m in highs]
            total = sum(r[8 + a : 9 + a, :] * n for (r, a), n in zip(held, ratio))
            f_ref[h * 4 + i : h * 4 + i + 1, :] = ratio[0] / total
    ones = jnp.ones((8, HEAD_DIM), flt)
    aq[...] = jnp.zeros_like(aq)
    ak[...] = jnp.zeros_like(ak)
    av[...] = jnp.zeros_like(av)
    heads = [slice(h * HEAD_DIM, (h + 1) * HEAD_DIM) for h in range(2)]
    for h, cols in enumerate(heads):
        for j, k_ref in enumerate((k0, k1, k2, k3)):
            kt[h * 4 + j] = k_ref[:, cols].T
    for i, (q_ref, o_ref) in enumerate(((q0, o0), (q1, o1), (q2, o2), (q3, o3))):
        g_ref = (g_mine, g_other)[i % 2]
        for h, cols in enumerate(heads):
            row = h * 4 + i
            prod = g_ref[i // 2, :, cols].astype(flt) * o_ref[:, cols].astype(flt)
            dl_ref[row : row + 1, :] = lax.dot_general(
                ones, prod, (((1,), (1,)), ((), ())),
                precision=lax.Precision.HIGHEST, preferred_element_type=flt,
            )[0:1]
            fetch(row).wait()
        for j, v_ref in enumerate((v0, v1, v2, v3)):

            @pl.when(bk_ref[j] <= bq_ref[i])
            def _():
                for h, cols in enumerate(heads):
                    row = h * 4 + i
                    g = g_ref[i // 2, :, cols]
                    w = e_now[row, j].astype(flt) * f_ref[row : row + 1, :]
                    d = nt(v_ref[:, cols], g)
                    ds = (w * (d - dl_ref[row : row + 1, :])).astype(half)
                    av[j, :, cols] += nn(w.astype(half), g)
                    ak[j, :, cols] += nn(ds, q_ref[:, cols])
                    aq[row] += nn(kt[h * 4 + j], ds)

    for h in range(2):
        cols = slice(h * HEAD_DIM, (h + 1) * HEAD_DIM)
        for i in range(4):
            got = aq[h * 4 + i].T * SCALE
            if i % 2:
                q_near[i // 2, :, cols] = got.astype(half)
            else:
                q_keep[i // 2, :, cols] = got
    for j, d_ref in enumerate((d0, d1, d2, d3)):
        d_ref[:, :256] = (ak[j] * SCALE).astype(half)
        d_ref[:, 256:] = av[j].astype(half)


def parts_kernel(r0, r1, r2, r3, wa, wb, out_ref):
    for b, w in enumerate((wa, wb)):
        for i, r in enumerate((r0, r1, r2, r3)):
            part = nt(r[...], w[...]).astype(half)
            out_ref[2 * i, :, b * 256 : (b + 1) * 256] = part[:128]
            out_ref[2 * i + 1, :, b * 256 : (b + 1) * 256] = part[128:]


def sums_kernel(y_ref, parts_ref, o0, o1, o2, o3):
    for n, out in enumerate((o0, o1, o2, o3)):
        at = pl.multiple_of(((y_ref[0] + n) % 4) * 32, 32)
        out[...] = jnp.sum(parts_ref[:, pl.ds(at, 32), :].astype(flt), axis=0).astype(half)


def copies_kernel(p0, p1, p2, p3, out_ref):
    for h in range(8):
        for n, p in enumerate((p0, p1, p2, p3)):
            out_ref[h, n * 32 : (n + 1) * 32, :] = p[...]


def natural_kernel(xh_ref, at_ref, lo_ref, hi_ref, w0, w1, w2, w3, nat_ref, keep_ref, send_ref, ws, full):
    for p, w in enumerate((w0, w1, w2, w3)):
        ws[:, p * 256 : (p + 1) * 256] = w[...]
    rows = lax.broadcasted_iota(jnp.int32, (512, 512), 0)
    for x in range(2):
        for z in range(4):
            at = z * 2 + (xh_ref[0] ^ x)
            for n in range(4):
                for ref, blocks in ((lo_ref, LOW), (hi_ref, HIGH)):
                    for b, m in enumerate(blocks):
                        p = (n + m) % 4
                        full[z * 128 + n * 32 : z * 128 + (n + 1) * 32, p * 256 : (p + 1) * 256] = ref[
                            at, n * 32 : (n + 1) * 32, b * 256 : (b + 1) * 256
                        ]
        hot = jnp.where(rows == at_ref[x : x + 1, :], 1.0, 0.0).astype(half)
        nat = nn(hot, full[...]).astype(half)
        nat_ref[x * 512 : (x + 1) * 512, :] = nat
        part = nt(nat, ws[...]).astype(half)
        keep_ref[x] = part[:256]
        send_ref[x] = part[256:]


def late_kernel(turn_ref, nat_ref, o0, o1, o2, o3, t0, t1, t2, t3, near_ref, other_ref, o):
    at = pl.multiple_of(turn_ref[0] * 256, 256)
    for x in range(2):
        near_ref[x] = nat_ref[x * 512 : x * 512 + 256, pl.ds(at, 256)]
        other_ref[x] = nat_ref[x * 512 + 256 : (x + 1) * 512, pl.ds(at, 256)]
    for i, r in enumerate((o0, o1, o2, o3)):
        o[i * 256 : (i + 1) * 256, :] = r[...]
    for n, t in enumerate((t0, t1, t2, t3)):
        p = (4 - n) % 4
        t[...] = tn(o[...], nat_ref[:, p * 256 : (p + 1) * 256]).astype(half)


def terms_kernel(at_ref, d0, d1, d2, d3, y0, y1, y2, y3, keep0, keep1, send):
    def part(a, b):
        at = pl.multiple_of((at_ref[0] ^ a) * 512 + (at_ref[1] ^ b) * 256, 256)
        total = None
        for d, r in ((d0, y0), (d1, y1), (d2, y2), (d3, y3)):
            now = tn(r[:, pl.ds(at, 256)], d[...])
            total = now if total is None else total + now
        return total.astype(half)

    keep0[...] = part(0, 0)
    keep1[...] = part(1, 0)
    send[0] = part(0, 1)
    send[1] = part(1, 1)


VMEM = pl.BlockSpec(memory_space=pltpu.VMEM)
SMEM = pl.BlockSpec(memory_space=pltpu.SMEM)
ANY = pl.BlockSpec(memory_space=pl.ANY)
HBM = pl.BlockSpec(memory_space=pltpu.HBM)


def columns(n):
    return [pl.BlockSpec((256, 256), lambda i: (0, n))] * 4


def cost(flops):
    return pl.CostEstimate(flops=flops, bytes_accessed=2**21, transcendentals=0)


def shaped(*shape, dtype=half):
    return jax.ShapeDtypeStruct(shape, dtype)


def call(kernel, out_shape, in_specs, flops, scratch=()):
    many = isinstance(out_shape, list)
    return pl.pallas_call(
        kernel,
        grid=(1,),
        out_shape=out_shape,
        in_specs=in_specs,
        out_specs=[VMEM] * len(out_shape) if many else VMEM,
        scratch_shapes=list(scratch),
        cost_estimate=cost(flops),
        compiler_params=pltpu.CompilerParams(vmem_limit_bytes=48 * 2**20),
    )


def stats_of(bq, bk, sides, kvw):
    return pl.pallas_call(
        stats_kernel,
        grid=(1,),
        out_shape=[shaped(16, 256, dtype=flt), shaped(32, 256, 256)],
        in_specs=[SMEM] * 2 + columns(0) + columns(0),
        out_specs=[VMEM, HBM],
        scratch_shapes=[
            pltpu.VMEM((8, 256, 256), flt),
            pltpu.VMEM((8, 4, 256, 256), half),
            pltpu.SemaphoreType.DMA((8,)),
        ],
        cost_estimate=cost(3 * 2**30),
        compiler_params=pltpu.CompilerParams(vmem_limit_bytes=48 * 2**20),
    )(bq, bk, *sides, *kvw)


def backward_of(bq, bk, sides, mine, other, kvw, stats, e):
    return call(
        backward_kernel,
        [shaped(2, 256, 256, dtype=flt), shaped(2, 256, 256)] + [shaped(256, 512)] * 4,
        [SMEM] * 2 + columns(0) + columns(1) + [VMEM] * 2 + columns(0) + columns(1) + [VMEM] * 4 + [ANY],
        6 * 2**30,
        [pltpu.VMEM((8, 256), flt)] * 2
        + [pltpu.VMEM((8, 128, 256), half), pltpu.VMEM((8, 128, 256), flt)]
        + [pltpu.VMEM((4, 256, 256), flt)] * 2
        + [pltpu.VMEM((8, 4, 256, 256), half), pltpu.SemaphoreType.DMA((8,))],
    )(bq, bk, *sides, *sides, mine, other, *kvw, *kvw, *stats, e)


def parts_of(rows, wa, wb):
    return call(parts_kernel, shaped(8, 128, 512), [VMEM] * 6, 2**30)(*rows, wa, wb)


def sums_of(y, parts):
    return call(sums_kernel, [shaped(32, 512)] * 4, [SMEM, VMEM], 2**26)(y, parts)


def copies_of(pieces):
    return call(copies_kernel, shaped(8, 128, 512), [VMEM] * 4, 2**26)(*pieces)


def natural_of(xh, at, lo, hi, kvw):
    return call(
        natural_kernel,
        [shaped(1024, 1024), shaped(2, 256, 256), shaped(2, 256, 256)],
        [SMEM] + [VMEM] * 3 + columns(2),
        2 * 2**30,
        [pltpu.VMEM((256, 1024), half), pltpu.VMEM((512, 1024), half)],
    )(xh, at, lo, hi, *kvw)


def late_of(turn, natural, sides):
    return call(
        late_kernel,
        [shaped(256, 256)] * 4 + [shaped(2, 256, 256)] * 2,
        [SMEM, VMEM] + columns(1),
        2**30,
        [pltpu.VMEM((1024, 256), half)],
    )(turn, natural, *sides)


def terms_of(at, ds, ys):
    return call(
        terms_kernel,
        [shaped(256, 1024)] * 2 + [shaped(2, 256, 1024)],
        [SMEM] + [VMEM] * 8,
        3 * 2**30,
    )(at, *ds, *ys)


LOW, HIGH = (0, 1), (3, 2)


def exchanged(x, axes):
    return lax.all_to_all(x, axes, 0, 0, tiled=True)


def moved(x, axis, k=1):
    return shift(x, axis, k)


def around(xs, axis, sign=1):
    xs = list(xs) if isinstance(xs, (list, tuple)) else [xs] * 4
    got = {m: moved(xs[m], axis, sign * m) for m in (1, 3, 2)}
    return [xs[0], got[1], got[2], got[3]]


def after(first, parts):
    return lax.optimization_barrier((first, *parts))[1:]


def body(d_bytes, owner_groups, block_order, y_in, w_proj, w_out, queries, keys, values, attn_out):
    y, xh, c, z, xl = (lax.axis_index(a) for a in ("y", "xh", "c", "z", "xl"))
    q = xh * 2 + c
    s = y * 4 + q
    i4 = jnp.arange(4, dtype=jnp.int32)
    i16 = jnp.arange(16, dtype=jnp.int32)
    seq, head = ("y", "xh", "c"), ("z", "xl")
    one = lambda t: t.reshape(1).astype(jnp.int32)

    mine = dyn(owner_groups, s) // 16
    place = ((mine // 2) % 2) * 8 + (mine // 4) * 2 + mine % 2
    own = dot16(one_hot_rows(in_group(place, 16), 256), d_bytes, 1, 0)
    r10 = moved(own, "xh")
    w_rel = around(w_proj, "y")
    r01 = moved(own, "c")
    r11 = moved(r10, "c")
    rows = (own, r01, r10, r11)

    landing = jnp.sum(
        jnp.where(owner_groups[:, :, None] // 16 == i16, owner_groups[:, :, None] % 16, 0), axis=1
    )

    by_shard = dot16(one_hot_rows(in_group(mine, 16), 256), d_bytes, 1, 0)
    by_owner = exchanged(by_shard.reshape(16, 16, 1024), seq).reshape(256, 1024)
    kept = dot16(one_hot_rows(in_group(dyn(landing, s, 1), 16), 256), by_owner, 1, 0)
    d_near = around(kept, "y")
    y_cut = [lax.dynamic_slice_in_dim(y_in, ((y + n) % 4) * 1024, 1024, 1) for n in range(4)]

    def reduced(part):
        pieces = sums_of(one(y), exchanged(part, head))
        pieces = around(pieces, "y")
        return exchanged(copies_of(pieces), head)

    part = parts_of(rows, *[w_rel[m] for m in HIGH])
    part, *y_cut = lax.optimization_barrier((part, *y_cut))
    lo, hi = reduced(parts_of(rows, *[w_rel[m] for m in LOW])), reduced(part)
    y_near = around(y_cut, "y")

    src = jnp.arange(32, dtype=jnp.int32)
    owner = ((y - (src // 2) % 4) % 4) * 4 + (q ^ (src // 8))
    to_shard = y * 4 + (xh ^ jnp.arange(2, dtype=jnp.int32))[:, None] * 2 + (src % 2)[None, :]
    at = landing.reshape(-1)[owner[None, :] * 16 + to_shard] + ((src % 2) ^ c)[None, :] * 16

    side = jnp.concatenate([queries, attn_out], axis=1)
    s10 = moved(side, "xh")
    sides = (side, moved(side, "c"), s10, moved(s10, "c"))
    kvw = around(jnp.concatenate([keys, values, w_out], axis=1), "y")

    bq = block_order[y * 4 + (q ^ i4)]
    bk = block_order[((y - i4) % 4) * 4 + q]
    stats, e = stats_of(bq, bk, sides, kvw)
    far = lax.ppermute(stats, ("xh", "c"), [(i, i ^ 3) for i in range(4)])
    stats = (stats, moved(stats, "c"), moved(stats, "xh"), far)

    natural, keep, send = natural_of(one(xh), in_group(at, 32), lo, hi, kvw)
    grad = added(keep, moved(send, "c"))
    grad = added(grad, moved(grad, "xh")[::-1])
    q_keep, q_near, *dkv = backward_of(bq, bk, sides, grad, moved(grad, "c"), kvw, stats, e)
    dkv = around(dkv, "y", -1)
    q_far = moved(q_near, "c")
    q_send = added(q_keep[1], q_far[1])
    q_got = moved(q_send, "xh")
    dq = added(q_keep[0], q_far[0], q_got)

    *term, near, other = late_of(one((y - z) % 4), natural, sides)
    other = moved(other, "c")
    both = [
        jnp.concatenate(
            [jnp.where(c == 0, near[x], other[x]), jnp.where(c == 0, other[x], near[x])], axis=1
        )
        for x in range(2)
    ]
    both[1] = lax.ppermute(both[1], ("xh", "xl"), [(0, 2), (3, 1)])
    layer_grad = jnp.where(xh == xl, *both)
    grad_out = added(*after(q_send, around(term, "y")))

    keep0, keep1, send = terms_of(jnp.stack([xh, c]).astype(jnp.int32), d_near, y_near)
    got = moved(send, "c")
    far = moved(added(keep1, got[1]), "xh")
    grad_proj = added(*after(q_send, (keep0, got[0], far)))
    dkv = after(grad_proj, dkv)
    grad_keys = added(*[t[:, :256] for t in dkv])
    grad_values = added(*[t[:, 256:] for t in dkv])
    return layer_grad, grad_proj, grad_out, dq, grad_keys, grad_values


def solution(mesh):
    axes = ("y", "xh", "c", "z", "xl")
    finer = Mesh(mesh.devices.reshape([SIZE[a] for a in axes]), axes)
    seq, head = ("y", "xh", "c"), ("z", "xl")
    both = P(seq, head)
    placed = (both, P(), P(), P(seq, None), both, P(head, seq), both, both, both, both)
    return jax.shard_map(
        body,
        mesh=finer,
        in_specs=placed,
        out_specs=(both, both, P(head, seq), both, both, both),
        check_vma=False,
    )
```
